16 devices in a mesh: ep: 16 (over z, y, x, core).
Axes of the slice: x: 2, y: 2, z: 2, core: 2. Of those that a mesh axis runs over, the one named last changes fastest.
Arguments:
- x_tokens: bfloat16 [32768, 1536], P('ep')
- w_router: bfloat16 [1536, 64], replicated
- w_gate: bfloat16 [64, 1536, 512], P('ep')
- w_up: bfloat16 [64, 1536, 512], P('ep')
- w_down: bfloat16 [64, 512, 1536], P('ep')
- topk_idx: int32 [32768, 6], P('ep')
- dy_tokens: bfloat16 [32768, 1536], P('ep')
Outputs:
- output 1: bfloat16 [32768, 1536], P('ep')
- output 2: float32 [], replicated
- output 3: bfloat16 [32768, 1536], P('ep')
- output 4: float32 [1536, 64], replicated
- output 5: float32 [64, 1536, 512], P('ep')
- output 6: float32 [64, 1536, 512], P('ep')
- output 7: float32 [64, 512, 1536], P('ep')
All inputs are finite; a program needn't handle non-finite values.
Results may differ from the reference program's by a relative error of at most 0.00530925.
Values are sent between devices in bfloat16 or wider.
A program may use at most 1 GiB of HBM per device.

```python
import jax
import jax.numpy as jnp
from jax import lax

MODEL_DIM = 1536
FF_DIM = 512
NUM_EXPERTS = 64
TOP_K = 6
TOK_PER_DEV = 2048
NUM_DEVICES = 16
ALL_TOKENS = NUM_DEVICES * TOK_PER_DEV
CAPACITY = (5 * TOK_PER_DEV * TOP_K + 4 * NUM_EXPERTS - 1) // (4 * NUM_EXPERTS)
AUX_COEF = 0.001


def draw_routing(key):
    bias_key, score_key = jax.random.split(key)
    dev_bias = jax.random.randint(bias_key, (NUM_DEVICES, 1, NUM_EXPERTS), 0, 61)
    scores = jax.random.randint(score_key, (NUM_DEVICES, TOK_PER_DEV, NUM_EXPERTS), 0, 1000)
    ranked = (scores + dev_bias) * NUM_EXPERTS + jnp.arange(NUM_EXPERTS, dtype=jnp.int32)
    chosen = lax.top_k(ranked, TOP_K)[1]
    return chosen.reshape(ALL_TOKENS, TOP_K).astype(jnp.int32)


def setup_inputs(seed: int = 0) -> dict:
    key_list = jax.random.split(jax.random.key(seed), 7)
    topk_idx = draw_routing(key_list[0])
    router_f = jax.random.normal(key_list[1], (MODEL_DIM, NUM_EXPERTS), jnp.float32) * MODEL_DIM ** -0.5
    chosen_hot = jnp.zeros((ALL_TOKENS, NUM_EXPERTS), jnp.float32).at[jnp.arange(ALL_TOKENS)[:, None], topk_idx].set(1.0)
    x_noise = jax.random.normal(key_list[2], (ALL_TOKENS, MODEL_DIM), jnp.float32)
    x_tokens = x_noise + 3.0 * jnp.dot(chosen_hot, router_f.T)
    w_gate = jax.random.normal(key_list[3], (NUM_EXPERTS, MODEL_DIM, FF_DIM), jnp.float32) * MODEL_DIM ** -0.5
    w_up = jax.random.normal(key_list[4], (NUM_EXPERTS, MODEL_DIM, FF_DIM), jnp.float32) * MODEL_DIM ** -0.5
    w_down = jax.random.normal(key_list[5], (NUM_EXPERTS, FF_DIM, MODEL_DIM), jnp.float32) * FF_DIM ** -0.5
    dy_tokens = jax.random.normal(key_list[6], (ALL_TOKENS, MODEL_DIM), jnp.float32)
    return {
        "x_tokens": x_tokens.astype(jnp.bfloat16),
        "w_router": router_f.astype(jnp.bfloat16),
        "w_gate": w_gate.astype(jnp.bfloat16),
        "w_up": w_up.astype(jnp.bfloat16),
        "w_down": w_down.astype(jnp.bfloat16),
        "topk_idx": topk_idx,
        "dy_tokens": dy_tokens.astype(jnp.bfloat16),
    }


def reference(x_tokens, w_router, w_gate, w_up, w_down, topk_idx, dy_tokens):
    logits = jnp.dot(x_tokens, w_router, preferred_element_type=jnp.float32)
    router_prob = jax.nn.softmax(logits, axis=-1)
    counts = jax.ops.segment_sum(jnp.ones((ALL_TOKENS * TOP_K,), jnp.float32), topk_idx.reshape(-1), num_segments=NUM_EXPERTS)
    load_frac = counts / (ALL_TOKENS * TOP_K)
    mean_prob = jnp.mean(router_prob, axis=0)
    aux_loss = AUX_COEF * NUM_EXPERTS * jnp.sum(load_frac * mean_prob)
    aux_grad = AUX_COEF * NUM_EXPERTS * load_frac / ALL_TOKENS
    w_gate32 = w_gate.astype(jnp.float32)
    w_up32 = w_up.astype(jnp.float32)
    w_down32 = w_down.astype(jnp.float32)
    zero_row = jnp.zeros((1, MODEL_DIM), x_tokens.dtype)
    n_slots = NUM_EXPERTS * CAPACITY

    def device_step(carry_acc, dev_in):
        dwg_acc, dwu_acc, dwd_acc, dwr_acc = carry_acc
        x_dev, prob_dev, idx_dev, dy_dev = dev_in
        pick_prob = jnp.take_along_axis(prob_dev, idx_dev, axis=1)
        pick_sum = jnp.sum(pick_prob, axis=1, keepdims=True)
        gate_f32 = pick_prob / pick_sum
        gate_bf = gate_f32.astype(jnp.bfloat16)
        choice_mask = idx_dev[:, :, None] == jnp.arange(NUM_EXPERTS)[None, None, :]
        expert_hot = jnp.sum(choice_mask.astype(jnp.int32), axis=1)
        earlier = jnp.cumsum(expert_hot, axis=0) - expert_hot
        position = jnp.take_along_axis(earlier, idx_dev, axis=1)
        slot_ids = jnp.where(position < CAPACITY, idx_dev * CAPACITY + position, n_slots)
        flat_slots = slot_ids.reshape(-1)
        x_rep = jnp.broadcast_to(x_dev[:, None, :], (TOK_PER_DEV, TOP_K, MODEL_DIM)).reshape(TOK_PER_DEV * TOP_K, MODEL_DIM)
        buf_x = jnp.zeros((n_slots + 1, MODEL_DIM), x_dev.dtype).at[flat_slots].set(x_rep)[:n_slots]
        buf_x32 = buf_x.reshape(NUM_EXPERTS, CAPACITY, MODEL_DIM).astype(jnp.float32)
        gate_pre = jnp.einsum("ecd,edf->ecf", buf_x32, w_gate32)
        up_pre = jnp.einsum("ecd,edf->ecf", buf_x32, w_up32)
        act_gate = jax.nn.silu(gate_pre)
        hidden = (act_gate * up_pre).astype(jnp.bfloat16).astype(jnp.float32)
        out_slot = jnp.einsum("ecf,efd->ecd", hidden, w_down32).astype(jnp.bfloat16)
        out_tok = jnp.concatenate([out_slot.reshape(n_slots, MODEL_DIM), zero_row])[slot_ids]
        y_dev = jnp.sum(gate_bf.astype(jnp.float32)[:, :, None] * out_tok.astype(jnp.float32), axis=1).astype(jnp.bfloat16)
        do_tok = (gate_bf.astype(jnp.float32)[:, :, None] * dy_dev.astype(jnp.float32)[:, None, :]).astype(jnp.bfloat16)
        buf_do = jnp.zeros((n_slots + 1, MODEL_DIM), dy_dev.dtype).at[flat_slots].set(do_tok.reshape(TOK_PER_DEV * TOP_K, MODEL_DIM))[:n_slots]
        buf_do32 = buf_do.reshape(NUM_EXPERTS, CAPACITY, MODEL_DIM).astype(jnp.float32)
        dwd_new = dwd_acc + jnp.einsum("ecf,ecd->efd", hidden, buf_do32)
        d_hidden = jnp.einsum("ecd,efd->ecf", buf_do32, w_down32).astype(jnp.bfloat16).astype(jnp.float32)
        sigmoid_g = jax.nn.sigmoid(gate_pre)
        d_gate_pre = (d_hidden * up_pre * sigmoid_g * (1.0 + gate_pre * (1.0 - sigmoid_g))).astype(jnp.bfloat16).astype(jnp.float32)
        d_up_pre = (d_hidden * act_gate).astype(jnp.bfloat16).astype(jnp.float32)
        dwg_new = dwg_acc + jnp.einsum("ecd,ecf->edf", buf_x32, d_gate_pre)
        dwu_new = dwu_acc + jnp.einsum("ecd,ecf->edf", buf_x32, d_up_pre)
        dx_slot = (jnp.einsum("ecf,edf->ecd", d_gate_pre, w_gate32) + jnp.einsum("ecf,edf->ecd", d_up_pre, w_up32)).astype(jnp.bfloat16)
        dx_tok = jnp.concatenate([dx_slot.reshape(n_slots, MODEL_DIM), zero_row])[slot_ids]
        dx_expert = jnp.sum(dx_tok.astype(jnp.float32), axis=1)
        d_gate = jnp.sum(out_tok.astype(jnp.float32) * dy_dev.astype(jnp.float32)[:, None, :], axis=2)
        d_pick = (d_gate - jnp.sum(d_gate * gate_f32, axis=1, keepdims=True)) / pick_sum
        d_prob = jnp.sum(jnp.where(choice_mask, d_pick[:, :, None], 0.0), axis=1) + aux_grad
        d_logit = prob_dev * (d_prob - jnp.sum(prob_dev * d_prob, axis=1, keepdims=True))
        d_logit_bf = d_logit.astype(jnp.bfloat16)
        dwr_new = dwr_acc + jnp.dot(x_dev.T, d_logit_bf, preferred_element_type=jnp.float32)
        dx_dev = (dx_expert + jnp.dot(d_logit_bf, w_router.T, preferred_element_type=jnp.float32)).astype(jnp.bfloat16)
        return (dwg_new, dwu_new, dwd_new, dwr_new), (y_dev, dx_dev)

    init_acc = (
        jnp.zeros((NUM_EXPERTS, MODEL_DIM, FF_DIM), jnp.float32),
        jnp.zeros((NUM_EXPERTS, MODEL_DIM, FF_DIM), jnp.float32),
        jnp.zeros((NUM_EXPERTS, FF_DIM, MODEL_DIM), jnp.float32),
        jnp.zeros((MODEL_DIM, NUM_EXPERTS), jnp.float32),
    )
    dev_inputs = (
        x_tokens.reshape(NUM_DEVICES, TOK_PER_DEV, MODEL_DIM),
        router_prob.reshape(NUM_DEVICES, TOK_PER_DEV, NUM_EXPERTS),
        topk_idx.reshape(NUM_DEVICES, TOK_PER_DEV, TOP_K),
        dy_tokens.reshape(NUM_DEVICES, TOK_PER_DEV, MODEL_DIM),
    )
    final_acc, dev_outs = lax.scan(device_step, init_acc, dev_inputs)
    y_tokens = dev_outs[0].reshape(ALL_TOKENS, MODEL_DIM)
    dx_tokens = dev_outs[1].reshape(ALL_TOKENS, MODEL_DIM)
    return (y_tokens, aux_loss, dx_tokens, final_acc[3], final_acc[0], final_acc[1], final_acc[2])
```

```python
import functools

import jax
import jax.numpy as jnp
from jax import lax
from jax.experimental import pallas as pl
from jax.experimental.pallas import tpu as pltpu
from jax.sharding import PartitionSpec as P

AUX_COEF = 0.001
BF = jnp.bfloat16
F32 = jnp.float32
BLK = 256
WIN = 64
VMEM_LIMIT = 64_000_000


def dot(a, b, dims=((1,), (0,))):
    return lax.dot_general(a, b, (dims, ((), ())), preferred_element_type=F32)


def params(n_axes):
    return pltpu.CompilerParams(dimension_semantics=("arbitrary",) * n_axes, vmem_limit_bytes=VMEM_LIMIT)


def cost(flops, nbytes):
    return pl.CostEstimate(flops=int(flops), bytes_accessed=int(nbytes), transcendentals=0)


def build_hot(a_ref, slot_ref, wgt_ref, base_ref, s, blk, rnd, n_exp, n_blk, cap):
    iota = lax.broadcasted_iota(jnp.int32, (WIN, BLK), 0)
    cols = pl.ds(pl.multiple_of(blk * BLK, BLK), BLK)
    starts = []
    for e in range(n_exp):
        first = base_ref[(s * n_exp + e) * n_blk + blk] + rnd * WIN
        start = pl.multiple_of(jnp.minimum(first, cap - WIN), 16)
        starts.append(start)
        slot = slot_ref[0, pl.ds(e, 1), cols]
        rel = jnp.where(slot >= first, slot - start, -1)
        if wgt_ref is None:
            val = jnp.ones((), F32)
        else:
            val = wgt_ref[0, pl.ds(e, 1), cols]
        a_ref[pl.ds(e * WIN, WIN), :] = jnp.where(iota == rel, val, 0.0).astype(BF)
    return starts


def gather_kernel(n_exp, n_blk, cap, with_w, base_ref, rnds_ref, pos_ref, x_ref, slot_ref, *rest):
    if with_w:
        wgt_ref, out_ref, wcol_ref, a_ref = rest
    else:
        out_ref, a_ref = rest
    s = pl.program_id(0)
    out_ref[...] = jnp.zeros_like(out_ref)
    if with_w:
        wcol_ref[...] = jnp.zeros_like(wcol_ref)
    dim = x_ref.shape[-1]

    def block(blk, _):
        def one_round(rnd, _):
            starts = build_hot(a_ref, slot_ref, None, base_ref, s, blk, rnd, n_exp, n_blk, cap)
            rows = pl.ds(pl.multiple_of(blk * BLK, BLK), BLK)
            if with_w:
                for e in range(n_exp):
                    w_row = wgt_ref[0, pl.ds(e, 1), rows]
                    part = jnp.sum(a_ref[pl.ds(e * WIN, WIN), :].astype(F32) * w_row, axis=1, keepdims=True)
                    sel = pl.ds(starts[e], WIN)
                    wcol_ref[e, 0, sel, :] = wcol_ref[e, 0, sel, :] + jnp.broadcast_to(part, (WIN, 128))
            for n in range(dim // 256):
                lanes = pl.ds(n * 256, 256)
                res = dot(a_ref[...], x_ref[0, rows, lanes]).astype(BF)
                for e in range(n_exp):
                    sel = pl.ds(starts[e], WIN)
                    out_ref[e, 0, sel, lanes] = out_ref[e, 0, sel, lanes] + res[e * WIN:(e + 1) * WIN]
            return 0

        return lax.fori_loop(0, rnds_ref[s * n_blk + blk], one_round, 0)

    lax.fori_loop(0, n_blk, block, 0)


def gather_rows(x_all, slots, wgt, base, rnds, pos, cap):
    n_src, n_tok, dim = x_all.shape
    n_exp = slots.shape[1]
    n_blk = n_tok // BLK
    with_w = wgt is not None
    meta = pl.BlockSpec((1, n_exp, n_tok), lambda s, *_: (s, 0, 0))
    in_specs = [pl.BlockSpec((1, n_tok, dim), lambda s, b, r, p: (s ^ p[0], 0, 0)), meta]
    out_specs = [pl.BlockSpec((n_exp, 1, cap, dim), lambda s, *_: (0, s, 0, 0))]
    out_shape = [jax.ShapeDtypeStruct((n_exp, n_src, cap, dim), BF)]
    args = [x_all, slots]
    if with_w:
        in_specs.append(meta)
        args.append(wgt)
        out_specs.append(pl.BlockSpec((n_exp, 1, cap, 128), lambda s, *_: (0, s, 0, 0)))
        out_shape.append(jax.ShapeDtypeStruct((n_exp, n_src, cap, 128), F32))
    return pl.pallas_call(
        functools.partial(gather_kernel, n_exp, n_blk, cap, with_w),
        grid_spec=pltpu.PrefetchScalarGridSpec(
            num_scalar_prefetch=3,
            grid=(n_src,),
            in_specs=in_specs,
            out_specs=out_specs,
            scratch_shapes=[pltpu.VMEM((n_exp * WIN, BLK), BF)],
        ),
        out_shape=out_shape,
        compiler_params=params(1),
        cost_estimate=cost(2 * n_src * n_tok * n_exp * WIN * dim, 2 * n_src * (n_tok + n_exp * cap) * dim),
        name="gather_dy" if with_w else "gather_x",
    )(base, rnds, pos, *args)


def combine_kernel(n_grp, n_blk, cap, with_a, base_ref, rnds_ref, pos_ref, slot_ref, wgt_ref, *rest):
    rows_refs = rest[:n_grp]
    if with_a:
        acol_ref, out_ref, atok_ref, a_ref, win_ref = rest[n_grp:]
    else:
        out_ref, a_ref, win_ref = rest[n_grp:]
    s = pl.program_id(0)
    per = rows_refs[0].shape[0]
    n_exp = n_grp * per
    dim = out_ref.shape[-1]

    def block(blk, _):
        rows = pl.ds(pl.multiple_of(blk * BLK, BLK), BLK)

        def one_round(rnd, _):
            starts = build_hot(a_ref, slot_ref, None if with_a else wgt_ref, base_ref, s, blk, rnd, n_exp, n_blk, cap)
            for e in range(n_exp):
                win_ref[pl.ds(e * WIN, WIN), :] = rows_refs[e // per][e % per, 0, pl.ds(starts[e], WIN), :]
            if with_a:
                for e in range(n_exp):
                    col = acol_ref[e, 0, pl.ds(starts[e], WIN), :]
                    part = a_ref[pl.ds(e * WIN, WIN), :].astype(F32) * jnp.concatenate([col, col], axis=1)
                    part = jnp.sum(part, axis=0, keepdims=True)

                    @pl.when(rnd == 0)
                    def _():
                        atok_ref[0, pl.ds(e, 1), rows] = part

                    @pl.when(rnd > 0)
                    def _():
                        atok_ref[0, pl.ds(e, 1), rows] = atok_ref[0, pl.ds(e, 1), rows] + part

            for n in range(dim // 256):
                lanes = pl.ds(n * 256, 256)
                res = dot(a_ref[...], win_ref[:, lanes], ((0,), (0,)))

                @pl.when(rnd == 0)
                def _():
                    out_ref[0, rows, lanes] = res

                @pl.when(rnd > 0)
                def _():
                    out_ref[0, rows, lanes] = out_ref[0, rows, lanes] + res

            return 0

        return lax.fori_loop(0, rnds_ref[s * n_blk + blk], one_round, 0)

    lax.fori_loop(0, n_blk, block, 0)


def combine_rows(groups, slots, wgt, acol, base, rnds, pos, cap):
    n_src, n_exp, n_tok = slots.shape
    per = groups[0].shape[0]
    dim = groups[0].shape[-1]
    n_blk = n_tok // BLK
    with_a = acol is not None
    meta = pl.BlockSpec((1, n_exp, n_tok), lambda s, *_: (s, 0, 0))
    in_specs = [meta, meta] + [pl.BlockSpec((per, 1, cap, dim), lambda s, *_: (0, s, 0, 0))] * len(groups)
    args = [slots, wgt, *groups]
    out_specs = [pl.BlockSpec((1, n_tok, dim), lambda s, b, r, p: (s ^ p[0], 0, 0))]
    out_shape = [jax.ShapeDtypeStruct((n_src, n_tok, dim), F32)]
    if with_a:
        in_specs.append(pl.BlockSpec((n_exp, 1, cap, 128), lambda s, *_: (0, s, 0, 0)))
        args.append(acol)
        out_specs.append(meta)
        out_shape.append(jax.ShapeDtypeStruct((n_src, n_exp, n_tok), F32))
    return pl.pallas_call(
        functools.partial(combine_kernel, len(groups), n_blk, cap, with_a),
        grid_spec=pltpu.PrefetchScalarGridSpec(
            num_scalar_prefetch=3,
            grid=(n_src,),
            in_specs=in_specs,
            out_specs=out_specs,
            scratch_shapes=[pltpu.VMEM((n_exp * WIN, BLK), BF), pltpu.VMEM((n_exp * WIN, dim), BF)],
        ),
        out_shape=out_shape,
        compiler_params=params(1),
        cost_estimate=cost(2 * n_src * n_tok * n_exp * WIN * dim, n_src * (4 * n_tok + 2 * n_exp * cap) * dim),
        name="combine_dx" if with_a else "combine_y",
    )(base, rnds, pos, *args)


def fwd_kernel(tile, x_ref, wg_ref, wu_ref, wd_ref, g_ref, u_ref, h_ref, o_ref):
    def step(i, _):
        rows = pl.ds(pl.multiple_of(i * tile, tile), tile)
        x = x_ref[0, rows, :]
        g = dot(x, wg_ref[0])
        u = dot(x, wu_ref[0])
        g_ref[0, rows, :] = g
        u_ref[0, rows, :] = u
        h = (g * jax.nn.sigmoid(g) * u).astype(BF)
        h_ref[0, rows, :] = h
        o_ref[0, rows, :] = dot(h, wd_ref[0]).astype(BF)
        return 0

    lax.fori_loop(0, x_ref.shape[1] // tile, step, 0)


def expert_fwd(xs, off, wg, wu, wd):
    _, rows, dim = xs.shape
    n, _, ff = wg.shape
    tile = rows // 4
    at = lambda e: (e, 0, 0)
    return pl.pallas_call(
        functools.partial(fwd_kernel, tile),
        grid=(n,),
        in_specs=[
            pl.BlockSpec((1, rows, dim), lambda e: (e + off, 0, 0)),
            pl.BlockSpec((1, dim, ff), at),
            pl.BlockSpec((1, dim, ff), at),
            pl.BlockSpec((1, ff, dim), at),
        ],
        out_specs=[
            pl.BlockSpec((1, rows, ff), at),
            pl.BlockSpec((1, rows, ff), at),
            pl.BlockSpec((1, rows, ff), at),
            pl.BlockSpec((1, rows, dim), at),
        ],
        out_shape=[
            jax.ShapeDtypeStruct((n, rows, ff), F32),
            jax.ShapeDtypeStruct((n, rows, ff), F32),
            jax.ShapeDtypeStruct((n, rows, ff), BF),
            jax.ShapeDtypeStruct((n, rows, dim), BF),
        ],
        compiler_params=params(1),
        cost_estimate=cost(6 * n * rows * dim * ff, n * (6 * dim * ff + 4 * rows * dim + 10 * rows * ff)),
        name="expert_fwd",
    )(xs, wg, wu, wd)


def bwd_kernel(tile, with_init, count, x_ref, dy_ref, wcol_ref, g_ref, u_ref, h_ref, o_ref, wg_ref, wu_ref, wd_ref, *rest):
    if with_init:
        ig_hbm, iu_hbm, id_hbm = rest[:3]
        rest = rest[3:]
    dx_ref, acol_ref, dwg_hbm, dwu_hbm, dwd_hbm, d_s, dg_s, du_s, up_s, down_s, out_sem = rest[:11]
    if with_init:
        iup_s, idown_s, in_sem = rest[11:]
    n_rows, dim = x_ref.shape[1:]
    n_wide = dim // 256
    e = pl.program_id(0)

    def outs(ex, i, slot):
        cols = pl.ds(pl.multiple_of(i * 256, 256), 256)
        return (
            pltpu.make_async_copy(up_s.at[slot, 0], dwg_hbm.at[ex, cols, :], out_sem.at[slot, 0]),
            pltpu.make_async_copy(up_s.at[slot, 1], dwu_hbm.at[ex, cols, :], out_sem.at[slot, 1]),
            pltpu.make_async_copy(down_s.at[slot], dwd_hbm.at[ex, :, cols], out_sem.at[slot, 2]),
        )

    def inits(ex, i, slot):
        cols = pl.ds(pl.multiple_of(i * 256, 256), 256)
        return (
            pltpu.make_async_copy(ig_hbm.at[ex, cols, :], iup_s.at[slot, 0], in_sem.at[slot, 0]),
            pltpu.make_async_copy(iu_hbm.at[ex, cols, :], iup_s.at[slot, 1], in_sem.at[slot, 1]),
            pltpu.make_async_copy(id_hbm.at[ex, :, cols], idown_s.at[slot], in_sem.at[slot, 2]),
        )

    if with_init:
        for cp in inits(e, 0, 0):
            cp.start()

    def step(i, _):
        rows = pl.ds(pl.multiple_of(i * tile, tile), tile)
        dy = dy_ref[0, rows, :].astype(F32)
        w = wcol_ref[0, rows, :]
        d = (dy * jnp.concatenate([w] * (dim // 128), axis=1)).astype(BF)
        d_s[rows, :] = d
        a = jnp.sum(o_ref[0, rows, :].astype(F32) * dy, axis=1, keepdims=True)
        acol_ref[0, rows, :] = jnp.broadcast_to(a, (tile, 128))
        dh = dot(d, wd_ref[0], ((1,), (1,))).astype(BF).astype(F32)
        g = g_ref[0, rows, :]
        u = u_ref[0, rows, :]
        sg = jax.nn.sigmoid(g)
        dg = (dh * u * sg * (1.0 + g * (1.0 - sg))).astype(BF)
        du = (dh * (g * sg)).astype(BF)
        dg_s[rows, :] = dg
        du_s[rows, :] = du
        dx = dot(dg, wg_ref[0], ((1,), (1,))) + dot(du, wu_ref[0], ((1,), (1,)))
        dx_ref[0, rows, :] = dx.astype(BF)
        return 0

    lax.fori_loop(0, n_rows // tile, step, 0)

    def wide(i, _):
        slot = i % 2
        cols = pl.ds(pl.multiple_of(i * 256, 256), 256)

        @pl.when((i >= 2) | (e > 0))
        def _():
            for cp in outs(e, i, slot):
                cp.wait()

        xt = x_ref[0, :, cols]
        rg = dot(xt, dg_s[...], ((0,), (0,)))
        ru = dot(xt, du_s[...], ((0,), (0,)))
        rd = dot(h_ref[0], d_s[:, cols], ((0,), (0,)))
        if with_init:

            @pl.when(i + 1 < n_wide)
            def _():
                for cp in inits(e, i + 1, 1 - slot):
                    cp.start()

            for cp in inits(e, i, slot):
                cp.wait()
            rg = rg + iup_s[slot, 0]
            ru = ru + iup_s[slot, 1]
            rd = rd + idown_s[slot]
        up_s[slot, 0] = rg
        up_s[slot, 1] = ru
        down_s[slot] = rd
        for cp in outs(e, i, slot):
            cp.start()
        return 0

    lax.fori_loop(0, n_wide, wide, 0)

    @pl.when(e == count - 1)
    def _():
        for i in (n_wide - 2, n_wide - 1):
            for cp in outs(e, i, i % 2):
                cp.wait()


def expert_bwd(xs, dys, wcol, acts, ws, off, first, count, init=None):
    _, rows, dim = xs.shape
    wg, wu, wd = ws
    ff = wg.shape[2]
    tile = rows // 4
    full = lambda e: (e + off + first, 0, 0)
    grp = lambda e: (e + first, 0, 0)
    at = lambda e: (e, 0, 0)
    g, u, h, o = acts
    up_spec, down_spec = (1, dim, ff), (1, ff, dim)
    hbm = pl.BlockSpec(memory_space=pl.ANY)
    in_specs = [
        pl.BlockSpec((1, rows, dim), full),
        pl.BlockSpec((1, rows, dim), full),
        pl.BlockSpec((1, rows, 128), full),
        pl.BlockSpec((1, rows, ff), grp),
        pl.BlockSpec((1, rows, ff), grp),
        pl.BlockSpec((1, rows, ff), grp),
        pl.BlockSpec((1, rows, dim), grp),
        pl.BlockSpec(up_spec, grp),
        pl.BlockSpec(up_spec, grp),
        pl.BlockSpec(down_spec, grp),
    ]
    args = [xs, dys, wcol, g, u, h, o, wg, wu, wd]
    scratch = [
        pltpu.VMEM((rows, dim), BF),
        pltpu.VMEM((rows, ff), BF),
        pltpu.VMEM((rows, ff), BF),
        pltpu.VMEM((2, 2, 256, ff), F32),
        pltpu.VMEM((2, ff, 256), F32),
        pltpu.SemaphoreType.DMA((2, 3)),
    ]
    if init is not None:
        in_specs += [hbm, hbm, hbm]
        args += list(init)
        scratch += [
            pltpu.VMEM((2, 2, 256, ff), F32),
            pltpu.VMEM((2, ff, 256), F32),
            pltpu.SemaphoreType.DMA((2, 3)),
        ]
    return pl.pallas_call(
        functools.partial(bwd_kernel, tile, init is not None, count),
        grid=(count,),
        in_specs=in_specs,
        out_specs=[pl.BlockSpec((1, rows, dim), at), pl.BlockSpec((1, rows, 128), at), hbm, hbm, hbm],
        out_shape=[
            jax.ShapeDtypeStruct((count, rows, dim), BF),
            jax.ShapeDtypeStruct((count, rows, 128), F32),
            jax.ShapeDtypeStruct((count, dim, ff), F32),
            jax.ShapeDtypeStruct((count, dim, ff), F32),
            jax.ShapeDtypeStruct((count, ff, dim), F32),
        ],
        scratch_shapes=scratch,
        compiler_params=params(1),
        cost_estimate=cost(12 * count * rows * dim * ff, count * (18 * dim * ff + 8 * rows * dim + 10 * rows * ff)),
        name="expert_bwd",
    )(*args)


def solution(mesh):
    n_dev = mesh.shape["ep"]

    def swap(arr, bits):
        return lax.ppermute(arr, "ep", [(i, i ^ bits) for i in range(n_dev)])

    plane = [[z * 8 + y * 4 + x * 2 + c for y in range(2) for x in range(2)] for z in range(2) for c in range(2)]

    def local_block(x_loc, w_router, wg_loc, wu_loc, wd_loc, idx_loc, dy_loc):
        n_tok, dim = x_loc.shape
        top_k = idx_loc.shape[1]
        n_exp = w_router.shape[1]
        own = wg_loc.shape[0]
        ff = wg_loc.shape[2]
        cap = (5 * n_tok * top_k + 4 * n_exp - 1) // (4 * n_exp)
        n_total = n_tok * n_dev
        n_src, n_blk = 4, n_tok // BLK
        me = lax.axis_index("ep")
        pos = (me // 2) % 4

        def relabel(arr):
            arr = arr.reshape((2, 2, 2, 2, own) + arr.shape[1:])
            for axis in range(4):
                bit = (me // (8 >> axis)) % 2
                arr = jnp.where(bit == 1, jnp.flip(arr, axis), arr)
            return arr.reshape((n_exp,) + arr.shape[5:])

        x_all = lax.all_gather(x_loc, "ep", axis_index_groups=plane, tiled=False)
        dy_all = lax.all_gather(dy_loc, "ep", axis_index_groups=plane, tiled=False)

        ws = {0: (wg_loc, wu_loc, wd_loc)}
        ws[8] = tuple(swap(w, 8) for w in ws[0])
        ws[1] = tuple(swap(w, 1) for w in ws[0])
        ws[9] = tuple(swap(w, 1) for w in ws[8])
        order = (0, 1, 8, 9)

        wr_rel = relabel(w_router.T)
        logits = dot(wr_rel, x_loc, ((1,), (1,)))
        prob = jax.nn.softmax(logits, axis=0)
        idx_rel = idx_loc.T ^ (me * own)
        numbers = lax.broadcasted_iota(jnp.int32, (n_exp, n_tok), 0)
        hot = functools.reduce(jnp.logical_or, [numbers == idx_rel[k][None] for k in range(top_k)])
        hot_f = hot.astype(F32)
        tri = (lax.broadcasted_iota(jnp.int32, (n_tok, n_tok), 0) < lax.broadcasted_iota(jnp.int32, (n_tok, n_tok), 1)).astype(BF)
        earlier = dot(hot.astype(BF), tri)
        pick = jnp.where(hot, prob, 0.0)
        pick_sum = jnp.sum(pick, axis=0, keepdims=True)
        gate = pick / pick_sum
        slot = jnp.where(hot & (earlier < cap), earlier, -1.0).astype(BF)
        meta = jnp.stack([slot, gate.astype(BF)])
        meta = meta.reshape(2, 2, 2, 2, 2, own, n_tok).transpose(2, 3, 0, 1, 4, 5, 6).reshape(n_src, 2, 4 * own, n_tok)
        meta = jnp.stack([meta[0]] + [swap(meta[r], r * 2) for r in range(1, n_src)])
        slots = meta[:, 0].astype(F32).astype(jnp.int32)
        wgt = meta[:, 1].astype(F32)
        per_blk = jnp.sum((slots >= 0).astype(jnp.int32).reshape(n_src, 4 * own, n_blk, BLK), axis=3)
        upto = sum(jnp.pad(per_blk, ((0, 0), (0, 0), (b, 0)))[:, :, :n_blk] for b in range(n_blk))
        base = (upto - per_blk) // 16 * 16
        rnds = jnp.max(jnp.maximum((upto - base + WIN - 1) // WIN, 1), axis=1)
        base, rnds = base.reshape(-1), rnds.reshape(-1)
        pos_arr = pos.reshape(1)

        stats = jnp.concatenate([relabel(jnp.sum(hot_f, axis=1)), relabel(jnp.sum(prob, axis=1))])
        stats = lax.psum(stats, "ep")
        load_frac = stats[:n_exp] / (n_total * top_k)
        mean_prob = stats[n_exp:] / n_total
        aux_loss = AUX_COEF * n_exp * jnp.sum(load_frac * mean_prob)

        (xs,) = gather_rows(x_all, slots, None, base, rnds, pos_arr, cap)
        xs = xs.reshape(4 * own, n_src * cap, dim)
        acts = {r: expert_fwd(xs, i * own, *ws[r]) for i, r in enumerate(order)}
        outs = [acts[r][3].reshape(own, n_src, cap, dim) for r in order]
        (y_part,) = combine_rows(outs, slots, wgt, None, base, rnds, pos_arr, cap)
        y_loc = lax.psum_scatter(y_part, "ep", axis_index_groups=plane, tiled=False).astype(BF)

        dys, wcol = gather_rows(dy_all, slots, wgt, base, rnds, pos_arr, cap)
        dys = dys.reshape(4 * own, n_src * cap, dim)
        wcol = wcol.reshape(4 * own, n_src * cap, 128)

        def bwd(r, first, count, init=None):
            return expert_bwd(xs, dys, wcol, acts[r], ws[r], order.index(r) * own, first, count, init)

        parts = {r: [] for r in order}
        done = {}
        chunks = ((0, 1), (1, 1), (2, 2))
        for first, count in chunks:
            res = bwd(9, first, count)
            parts[9].append(res)
            done[first] = [swap(t, 1) for t in res[2:]]
        sent = []
        for first, count in chunks:
            res = bwd(8, first, count, done[first])
            parts[8].append(res)
            sent.append([swap(t, 8) for t in res[2:]])
        res = bwd(1, 0, own)
        parts[1].append(res)
        got = [swap(t, 1) for t in res[2:]]
        res = bwd(0, 0, own, got)
        parts[0].append(res)
        dws = []
        for i in range(3):
            dws.append(res[2 + i] + jnp.concatenate([s[i] for s in sent]))

        join = lambda r, i: parts[r][0][i] if len(parts[r]) == 1 else jnp.concatenate([p[i] for p in parts[r]])
        dxs = [join(r, 0).reshape(own, n_src, cap, dim) for r in order]
        acol = jnp.concatenate([join(r, 1) for r in order]).reshape(4 * own, n_src, cap, 128)
        dx_part, a_tok = combine_rows(dxs, slots, wgt, acol, base, rnds, pos_arr, cap)
        dx_exp = lax.psum_scatter(dx_part, "ep", axis_index_groups=plane, tiled=False)

        a_all = jnp.stack([a_tok[0]] + [swap(a_tok[r], r * 2) for r in range(1, n_src)])
        a_all = a_all.reshape(2, 2, 2, 2, own, n_tok).transpose(2, 0, 1, 3, 4, 5).reshape(n_exp, n_tok)
        d_pick = (a_all - jnp.sum(a_all * gate, axis=0, keepdims=True)) / pick_sum
        aux_grad = AUX_COEF * n_exp * relabel(load_frac) / n_total
        d_prob = jnp.where(hot, d_pick, 0.0) + aux_grad[:, None]
        d_logit = (prob * (d_prob - jnp.sum(prob * d_prob, axis=0, keepdims=True))).astype(BF)
        dwr = relabel(dot(d_logit, x_loc))
        for bits in (1, 2, 4, 8):
            dwr = dwr + swap(dwr, bits)
        dx_loc = (dx_exp + dot(d_logit, wr_rel, ((0,), (0,)))).astype(BF)
        return y_loc, aux_loss, dx_loc, dwr.T, dws[0], dws[1], dws[2]

    tok_spec = P("ep")
    return jax.shard_map(
        local_block,
        mesh=mesh,
        in_specs=(tok_spec, P(), tok_spec, tok_spec, tok_spec, tok_spec, tok_spec),
        out_specs=(tok_spec, P(), tok_spec, P(), tok_spec, tok_spec, tok_spec),
        check_vma=False,
    )
```
